32 devices in a mesh: gx: 8 (over y, x, core), gy: 4 (over z).
Axes of the slice: x: 2, y: 2, z: 4, core: 2. Of those that a mesh axis runs over, the one named last changes fastest.
Arguments:
- collocation: bfloat16 [3072, 16384], P(None, 'gx'), may hold values from -6 to 6
- density: bfloat16 [3072, 3072], P('gy'), may hold values from -0.109375 to 0.109375
- kernel: bfloat16 [16384, 8, 4, 512], P('gx', None, 'gy'), may hold values from -6.67572e-06 to 6.67572e-06
Outputs:
- exchange: float32 [3072, 3072], P('gx', 'gy')
The draws below stay inside these ranges and needn't reach their ends.
All inputs are finite; a program needn't handle non-finite values.
Results may differ from the reference program's by a relative error of at most 0.008.
Values may be sent and summed in bfloat16 or wider, within the bound.
A program may use at most 448 MiB of HBM per device.

```python
import jax
import jax.numpy as jnp
from jax import lax

NBF = 3072
NPTS = 16384
CYCLE_LEN = 8
COL_GROUPS = 4
PIECE = 512
N_GX = 8


def block_levels(stream_key, shape, pieces, smallest, high):
    factor_of, own = 1.0, jax.random.fold_in(stream_key, 6)
    for dim, blocks in pieces:
        steps = jnp.exp(jax.random.uniform(jax.random.fold_in(own, dim), (blocks,), jnp.float32, smallest / len(pieces), high / len(pieces)))
        factor_of = factor_of * jnp.repeat(steps, shape[dim] // blocks).reshape([-1 if axis == dim else 1 for axis in range(len(shape))])
    return factor_of


def noise(rng, shape, deviation, limit, cuts=(), held_as=jnp.bfloat16):
    values = deviation * jax.random.normal(rng, shape, jnp.float32)
    if cuts:
        values = values * block_levels(rng, shape, cuts, -0.22, 0.18)
    return jnp.clip(values, -limit, limit).astype(held_as)


def setup_inputs(seed: int = 0) -> dict:
    key_list = jax.random.split(jax.random.key(seed), 4)
    collocation = noise(key_list[0], (NBF, NPTS), 1.0, 6.0, ((1, 8),))
    density = noise(key_list[1], (NBF, NBF), NBF ** -0.5, 0.109375, ((0, 4),))
    kernel = noise(key_list[2], (NPTS, CYCLE_LEN, COL_GROUPS, PIECE), (NPTS * NPTS * NBF) ** -0.5, 6.67572021484375e-06, ((0, 8), (2, 4)))
    return {"collocation": collocation, "density": density, "kernel": kernel}


def reference(collocation, density, kernel):
    dense = jnp.dot(density, collocation, preferred_element_type=jnp.float32).astype(jnp.bfloat16)
    flat_kernel = kernel.reshape(NPTS, NPTS)
    block_len = NPTS // N_GX

    def scan_step(running, position):
        offset = (position * block_len).astype(jnp.int32)
        dense_rows = lax.dynamic_slice_in_dim(dense, offset, block_len, 1)
        colloc_rows = lax.dynamic_slice_in_dim(collocation, offset, block_len, 1)
        coefficients = lax.dynamic_slice_in_dim(flat_kernel, offset, block_len, 0)
        products = jnp.dot(dense_rows.T, collocation, preferred_element_type=jnp.float32)
        weighted = (coefficients.astype(jnp.float32) * products).astype(jnp.bfloat16)
        contracted = jnp.dot(weighted, collocation.T, preferred_element_type=jnp.float32).astype(jnp.bfloat16)
        return running + jnp.dot(colloc_rows, contracted, preferred_element_type=jnp.float32), None

    running, unused = lax.scan(scan_step, jnp.zeros((NBF, NBF), jnp.float32), jnp.arange(N_GX, dtype=jnp.int32))
    return running
```

```python
import functools
import math

import jax
import jax.numpy as jnp
from jax import lax
from jax.experimental import pallas as pl
from jax.experimental.pallas import tpu as pltpu
from jax.sharding import PartitionSpec as P

F32 = jnp.float32
BF16 = jnp.bfloat16
MESH = pl.DeviceIdType.MESH


def largest_tile(size, limit):
    tile = limit
    while size % tile:
        tile //= 2
    return tile


def plan(n_gx, n_gy, nbf, rows, piece):
    s = type("Plan", (), {})()
    s.n_gx, s.n_gy, s.nbf, s.rows, s.piece = n_gx, n_gy, nbf, rows, piece
    s.bits = int(math.log2(n_gx)) - 1
    assert 2 << s.bits == n_gx and s.bits >= 1
    s.chips = n_gx // 2
    s.halves = 2 if piece % 256 == 0 else 1
    s.cw = piece // s.halves
    s.plane = nbf // n_gy
    s.strip = s.plane // n_gx
    s.mb = nbf // n_gx
    s.ch = 128 * s.bits
    s.chunks = nbf // s.ch
    s.per_plane = s.plane // s.ch
    s.units = sorted(
        ((r, h) for r in range(n_gx) for h in range(s.halves)),
        key=lambda u: (bin(u[0] >> 1).count("1"), u[1] if u[0] > 1 else 0, u[0] & 1, u[0], u[1]),
    )
    s.k_all = n_gx * piece
    s.k_half = s.k_all // 2
    s.t_rows = max(rows, nbf // 2 + 2 * s.ch)
    s.pt = largest_tile(rows, 512)
    s.zr = largest_tile(rows, 64)
    return s


def last_bit(s, p, d):
    order = [(p + t) % s.bits for t in range(s.bits)]
    return [q for q in order if d >> q & 1][-1]


def kernel_body(s, coll, dens, zk, out, dfull, gath, coll_v, dt, w, gbuf, r0, r1, rz, zin, zf,
                keep, ks, uf, sem_z, sem_zs, sem_d, sem_ds, sem_g, sem_gs, sem_l, sem_gu, sem_zin,
                sem_rd, sem_rds, sem_rs, sem_rss, sem_rz, sem_rzs, ready):
    i, j = lax.axis_index("gx"), lax.axis_index("gy")
    bits, nbf, halves, cw, ch, mb = s.bits, s.nbf, s.halves, s.cw, s.ch, s.mb
    bit = [lax.rem(i // (1 << t), 2) for t in range(bits + 1)]

    def flip(mask):
        index = i
        for t in range(bits + 1):
            if mask >> t & 1:
                index = index + (1 - 2 * bit[t]) * (1 << t)
        return index

    def plane_at(shift):
        return lax.rem(j + shift + s.n_gy, s.n_gy)

    def rows_at(start, size, unit=8):
        return pl.ds(pl.multiple_of(start, unit), size)

    def remote(src, dst, send, recv, gx, gy):
        return pltpu.make_async_remote_copy(
            src_ref=src, dst_ref=dst, send_sem=send, recv_sem=recv,
            device_id=(gx, gy), device_id_type=MESH)

    def hop(p, r):
        if r & 1:
            return r - 1, 1
        q = last_bit(s, p, r >> 1)
        return r - (2 << q), 2 << q

    own_cols = j * s.piece

    def own_piece(h, rws):
        return coll.at[rws, rows_at(own_cols + h * cw, cw, 128)]

    part_rows = nbf // bits

    def g_copy(h, p, r):
        src_r, mask = hop(p, r)
        rws = pl.ds(p * part_rows, part_rows)
        src = own_piece(h, rws) if src_r == 0 else gath.at[src_r * halves + h, rws]
        return remote(src, gath.at[r * halves + h, rws],
                      sem_gs.at[h, p, r], sem_g.at[h, p, r], flip(mask), j)

    def d_copy(t, p, r):
        src_r, mask = hop(p, r)
        start = plane_at(-t) * s.plane + flip(src_r) * s.strip
        ref = dfull.at[rows_at(start, s.strip), pl.ds(p * part_rows, part_rows)]
        return remote(ref, ref, sem_ds.at[t, p, r], sem_d.at[t, p, r], flip(mask), j)

    def z_copy(t):
        src = dens.at[rows_at(i * s.strip, s.strip)]
        dst = dfull.at[rows_at(j * s.plane + i * s.strip, s.strip)]
        return remote(src, dst, sem_zs.at[t], sem_z.at[t], i, plane_at(t))

    def onward(make, d):
        for p in range(bits):
            make(p, 2 * d + 1).start()
        for p in range(bits):
            for r in range(2, s.n_gx, 2):
                if hop(p, r)[0] == 2 * d:
                    make(p, r).start()

    for t in range(1, s.n_gy):
        z_copy(t).start()
    load_coll = pltpu.make_async_copy(coll, coll_v, sem_l.at[0])
    load_coll.start()
    load_dens = pltpu.make_async_copy(dens, r0.at[pl.ds(0, s.plane)], sem_l.at[1])
    load_dens.start()
    for p in range(bits):
        g_copy(0, p, 2 << p).start()
    for h in range(halves):
        for p in range(bits):
            g_copy(h, p, 1).start()

    rt = largest_tile(s.plane, 256) if s.plane % 384 else 384

    def dense(mu0):
        def step(n, carry):
            a, t = lax.rem(n, s.plane // rt), n // (s.plane // rt)
            block = jnp.dot(r0[rows_at(a * rt, rt, 128), :], coll_v[:, rows_at(t * s.pt, s.pt, 128)],
                            preferred_element_type=F32)
            dt[rows_at(t * s.pt, s.pt, 128), rows_at(mu0 + a * rt, rt, 128)] = block.T.astype(BF16)
            return carry
        lax.fori_loop(0, (s.plane // rt) * (s.rows // s.pt), step, 0)

    def z_load(n):
        return pltpu.make_async_copy(zk.at[rows_at(n * s.zr, s.zr)], zin.at[lax.rem(n, 2)],
                                     sem_zin.at[lax.rem(n, 2)])

    def spread_kernel():
        steps = s.rows // s.zr
        lanes = s.piece // 128

        def step(n, carry):
            @pl.when(n + 1 < steps)
            def _():
                z_load(n + 1).start()
            z_load(n).wait()
            block = zin[lax.rem(n, 2)].astype(F32).reshape(s.zr * s.n_gx, s.piece)
            for c in range(lanes):
                zf[c] = block[:, c * 128:(c + 1) * 128]
            for u, (r, h) in enumerate(s.units):
                k = flip(r)
                for c in range(cw // 128):
                    lane = zf[h * (cw // 128) + c, pl.ds(k, s.zr, stride=s.n_gx), :]
                    w[rows_at(n * s.zr, s.zr, 16), pl.ds(u * cw + c * 128, 128)] = lane.astype(BF16)
            return carry
        lax.fori_loop(0, steps, step, 0)

    z_load(0).start()
    load_coll.wait()
    load_dens.wait()
    dense(j * s.plane)

    chip_order = sorted(range(1, s.chips), key=lambda d: (bin(d).count("1"), d))

    def strip_on(t):
        z_copy(t).wait_recv()
        onward(functools.partial(d_copy, t), 0)

    def strips_on(t):
        for d in chip_order:
            for p in range(bits):
                d_copy(t, p, 2 * d).wait_recv()
            onward(functools.partial(d_copy, t), d)

    def dense_of(t):
        for d in range(s.chips):
            for p in range(bits):
                d_copy(t, p, 2 * d + 1).wait_recv()
        mu0 = plane_at(-t) * s.plane
        load = pltpu.make_async_copy(dfull.at[rows_at(mu0, s.plane, 128)], r0.at[pl.ds(0, s.plane)],
                                     sem_l.at[1])
        load.start()
        load.wait()
        dense(mu0)

    for t in range(1, s.n_gy):
        strip_on(t)
        if t == 1:
            spread_kernel()
        if t >= 2:
            strips_on(t - 1)
        if t >= 3:
            dense_of(t - 2)
    strips_on(s.n_gy - 1)
    for h in range(halves):
        for p in range(bits):
            if h > 0:
                g_copy(h, p, 2 << p).start()
        for p in range(bits):
            for q in range(bits):
                if q != p:
                    g_copy(h, p, 2 << q).start()
    for t in range(max(1, s.n_gy - 2), s.n_gy):
        dense_of(t)

    def fetch(u):
        r, h = s.units[u]
        slot = gbuf.at[u % 2, pl.ds(0, nbf), pl.ds(0, cw)]
        if r == 0:
            src = own_piece(h, pl.ds(0, nbf))
        else:
            src = gath.at[r * halves + h]
        return pltpu.make_async_copy(src, slot, sem_l.at[2 + u % 2])

    def arrive(u):
        r, h = s.units[u]
        if r:
            for p in range(bits):
                g_copy(h, p, r).wait_recv()
        if r and not r & 1:
            onward(functools.partial(g_copy, h), r >> 1)
        fetch(u).start()

    arrive(0)
    n_units, tiles = len(s.units), s.rows // s.pt

    def m_step(n, carry):
        u, t = n // tiles, lax.rem(n, tiles)
        slot = lax.rem(u, 2)

        @pl.when(t == 0)
        def _():
            pltpu.make_async_copy(gath.at[0], gbuf.at[slot, pl.ds(0, nbf), pl.ds(0, cw)],
                                  sem_l.at[2 + slot]).wait()

        for uu in range(1, n_units):
            @pl.when(jnp.logical_and(t == tiles // 2, u + 1 == uu))
            def _():
                arrive(uu)

        products = jnp.dot(dt[rows_at(t * s.pt, s.pt, 128), :], gbuf[slot, :nbf, :cw],
                           preferred_element_type=F32)
        place = (rows_at(t * s.pt, s.pt, 128), rows_at(u * cw, cw, 128))
        w[place] = (w[place].astype(F32) * products).astype(BF16)
        return carry
    lax.fori_loop(0, n_units * tiles, m_step, 0)

    masks = [1] + [2 << q for q in range(bits)]
    for t, mask in enumerate(masks):
        pl.semaphore_signal(ready.at[t], inc=1, device_id=(flip(mask), j), device_id_type=MESH)

    def chunk_plane(n):
        shift = n // s.per_plane + 1
        return lax.rem(j + shift, s.n_gy)

    def gu_copies(n, part):
        nu0 = chunk_plane(n) * s.plane + lax.rem(n, s.per_plane) * ch
        rws = rows_at(nu0, ch, 128)
        half = n_units // 2
        for u in range(part * half, (part + 1) * half):
            r, h = s.units[u]
            if r == 0:
                src = own_piece(h, rws)
            else:
                src = gath.at[r * halves + h, rws]
            dst = dt.at[pl.ds(nbf // 2 + part * ch, ch), pl.ds((u - part * half) * cw, cw)]
            yield pltpu.make_async_copy(src, dst, sem_gu.at[part, u - part * half])

    for part in range(2):
        for copy in gu_copies(0, part):
            copy.start()
    for t in range(bits + 1):
        pl.semaphore_wait(ready.at[t], 1)

    half_rows = nbf // 2
    send_d = gbuf.at[0, pl.ds(0, half_rows), pl.ds(0, ch)]
    u_v = gbuf.at[1, pl.ds(0, s.rows), pl.ds(0, ch)]
    send_at, at = [], half_rows
    for t in range(bits):
        size = (s.chips >> (t + 1)) * mb
        send_at.append((at, size))
        at += size
    sz = gbuf.at[0, pl.ds(at, mb), pl.ds(0, ch)]
    assert at + mb <= nbf
    recvs = [r0] + [r1[t] for t in range(bits - 1)]

    def cols(n):
        return rows_at(n * ch, ch, 128)

    def swap_copy(n):
        return remote(send_d, dt.at[pl.ds(0, half_rows), cols(n)], sem_rds.at[0], sem_rd.at[n],
                      flip(1), j)

    def halve_copy(n, t, p):
        q = (p + t) % bits
        at, size = send_at[t]
        return remote(gbuf.at[0, pl.ds(at, size), pl.ds(p * 128, 128)],
                      recvs[t].at[pl.ds(0, size), rows_at(n * ch + p * 128, 128, 128)],
                      sem_rss.at[t, p], sem_rs.at[n, t, p], flip(2 << q), j)

    def blocks(t, p):
        q = (p + t) % bits
        free = [f for f in range(bits) if f not in [(p + e) % bits for e in range(t)]]
        rest = [f for f in free if f != q]
        pairs = []
        for combo in range(1 << len(rest)):
            base = 0
            for e, f in enumerate(rest):
                base = base + (combo >> e & 1) * (1 << free.index(f))
            weight = 1 << free.index(q)
            mine = bit[q + 1]
            pairs.append((base + mine * weight, base + (1 - mine) * weight))
        return pairs

    def halve(n, t):
        held = keep if t == 0 else ks[t - 1]
        at, _ = send_at[t]

        for p in range(bits):
            lane = pl.ds(p * 128, 128)

            @pl.when(n >= 1)
            def _():
                halve_copy(n - 1, t, p).wait_send()
            for e, (kept, sent) in enumerate(blocks(t, p)):
                gbuf[0, pl.ds(at + e * mb, mb), lane] = held[rows_at(sent * mb, mb, 128), lane].astype(BF16)
            halve_copy(n, t, p).start()
            for e, (kept, sent) in enumerate(blocks(t, p)):
                ks[t][pl.ds(e * mb, mb), lane] = held[rows_at(kept * mb, mb, 128), lane]

    def take(n, t):
        _, size = send_at[t]
        for p in range(bits):
            halve_copy(n, t, p).wait_recv()
            lane = pl.ds(p * 128, 128)
            ks[t][pl.ds(0, size), lane] += recvs[t][
                pl.ds(0, size), rows_at(n * ch + p * 128, 128, 128)].astype(F32)

    def plane_copy(n):
        shift = n // s.per_plane + 1
        c = lax.rem(n, s.per_plane)
        dst = rz.at[rows_at((shift - 1) * mb, mb, 8), rows_at(c * ch, ch, 128)]
        return remote(sz, dst, sem_rzs.at[0], sem_rz.at[n], i, chunk_plane(n))

    away = (s.n_gy - 1) * s.per_plane

    def finish(n):
        total = ks[bits - 1]

        @pl.when(n < away)
        def _():
            @pl.when(n >= 1)
            def _():
                plane_copy(n - 1).wait_send()
            sz[...] = total[pl.ds(0, mb), :].astype(BF16)
            plane_copy(n).start()

        @pl.when(n >= away)
        def _():
            c = n - away
            for t in range(s.n_gy - 1):
                plane_copy(t * s.per_plane + c).wait_recv()
                total[pl.ds(0, mb), :] += rz[pl.ds(t * mb, mb), cols(c)].astype(F32)
            copy = pltpu.make_async_copy(total.at[pl.ds(0, mb)], out.at[:, cols(c)], sem_l.at[0])
            copy.start()
            copy.wait()

    core = bit[0]

    def b_step(n, carry):
        @pl.when(n < s.chunks)
        def _():
            for part in range(2):
                for copy in gu_copies(n, part):
                    copy.wait()

                def u_step(t, carry):
                    rws = rows_at(t * s.pt, s.pt, 128)
                    piece = lax.dot_general(
                        w[rws, pl.ds(part * s.k_half, s.k_half)],
                        dt[pl.ds(nbf // 2 + part * ch, ch), pl.ds(0, s.k_half)],
                        (((1,), (1,)), ((), ())), preferred_element_type=F32)
                    if part == 0:
                        uf[rws, :] = piece
                    else:
                        gbuf[1, rws, pl.ds(0, ch)] = (uf[rws, :] + piece).astype(BF16)
                    return carry
                lax.fori_loop(0, tiles, u_step, 0)

                @pl.when(n + 1 < s.chunks)
                def _():
                    for copy in gu_copies(n + 1, part):
                        copy.start()

        for t in reversed(range(bits)):
            m = n - 2 - t

            @pl.when(jnp.logical_and(m >= 0, m < s.chunks))
            def _():
                take(m, t)
                if t == bits - 1:
                    finish(m)
                else:
                    halve(m, t + 1)

        @pl.when(jnp.logical_and(n >= 1, n <= s.chunks))
        def _():
            swap_copy(n - 1).wait()
            keep[...] += dt[pl.ds(0, half_rows), cols(n - 1)].astype(F32)
            halve(n - 1, 0)

        @pl.when(n < s.chunks)
        def _():
            def t_block(q, side):
                return jnp.dot(coll_v[rows_at((2 * q + side) * mb, mb, 128), :],
                               gbuf[1, pl.ds(0, s.rows), pl.ds(0, ch)], preferred_element_type=F32)

            def sent(q, carry):
                gbuf[0, rows_at(q * mb, mb, 128), pl.ds(0, ch)] = t_block(q, 1 - core).astype(BF16)
                return carry
            lax.fori_loop(0, s.chips, sent, 0)
            swap_copy(n).start()

            def kept(q, carry):
                keep[rows_at(q * mb, mb, 128), :] = t_block(q, core)
                return carry
            lax.fori_loop(0, s.chips, kept, 0)
        return carry
    lax.fori_loop(0, s.chunks + bits + 1, b_step, 0)

    plane_copy(away - 1).wait_send()
    for t in range(bits):
        for p in range(bits):
            halve_copy(s.chunks - 1, t, p).wait_send()
    for t in range(1, s.n_gy):
        z_copy(t).wait_send()
    for r in range(1, s.n_gx):
        for p in range(bits):
            for t in range(1, s.n_gy):
                d_copy(t, p, r).wait_send()
            for h in range(halves):
                g_copy(h, p, r).wait_send()


def build(n_gx, n_gy):
    def local(collocation, density, kernel):
        nbf, rows = collocation.shape
        s = plan(n_gx, n_gy, nbf, rows, kernel.shape[3])
        zk = kernel.reshape(rows, n_gx, kernel.shape[3])
        any_spec = pl.BlockSpec(memory_space=pl.ANY)
        dma = pltpu.SemaphoreType.DMA
        wide = max(s.cw, s.ch)
        r1 = [pltpu.VMEM(((s.chips >> (t + 1)) * s.mb, nbf), BF16) for t in range(1, s.bits)]
        ks = [pltpu.VMEM(((s.chips >> (t + 1)) * s.mb, s.ch), F32) for t in range(s.bits)]
        out = pl.pallas_call(
            functools.partial(kernel_body, s),
            out_shape=(
                jax.ShapeDtypeStruct((s.mb, s.plane), F32),
                jax.ShapeDtypeStruct((nbf, nbf), BF16),
                jax.ShapeDtypeStruct((n_gx * s.halves, nbf, s.cw), BF16),
            ),
            in_specs=[any_spec] * 3,
            out_specs=(any_spec,) * 3,
            scratch_shapes=[
                pltpu.VMEM((nbf, rows), BF16),
                pltpu.VMEM((s.t_rows, nbf), BF16),
                pltpu.VMEM((rows, s.k_all), BF16),
                pltpu.VMEM((2, nbf, wide), BF16),
                pltpu.VMEM((max(s.plane, (s.chips // 2) * s.mb), nbf), BF16),
                r1,
                pltpu.VMEM(((n_gy - 1) * s.mb, s.plane), BF16),
                pltpu.VMEM((2, s.zr, n_gx, s.piece), BF16),
                pltpu.VMEM((s.piece // 128, s.zr * n_gx, 128), F32),
                pltpu.VMEM((nbf // 2, s.ch), F32),
                ks,
                pltpu.VMEM((rows, s.ch), F32),
                dma((n_gy,)),
                dma((n_gy,)),
                dma((n_gy, s.bits, n_gx)),
                dma((n_gy, s.bits, n_gx)),
                dma((s.halves, s.bits, n_gx)),
                dma((s.halves, s.bits, n_gx)),
                dma((4,)),
                dma((2, len(s.units) // 2)),
                dma((2,)),
                dma((s.chunks,)),
                dma((1,)),
                dma((s.chunks, s.bits, s.bits)),
                dma((s.bits, s.bits)),
                dma((s.chunks,)),
                dma((1,)),
                pltpu.SemaphoreType.REGULAR((s.bits + 1,)),
            ],
            compiler_params=pltpu.CompilerParams(
                has_side_effects=True, vmem_limit_bytes=67043328),
            name="exchange",
        )(collocation, density, zk)
        return out[0]

    return local


def solution(mesh):
    return jax.shard_map(
        build(mesh.shape["gx"], mesh.shape["gy"]),
        mesh=mesh,
        in_specs=(P(None, "gx"), P("gy", None), P("gx", None, "gy", None)),
        out_specs=P("gx", "gy"),
        check_vma=False,
    )
```

```python
import functools
import math

import jax
import jax.numpy as jnp
from jax import lax
from jax.experimental import pallas as pl
from jax.experimental.pallas import tpu as pltpu
from jax.sharding import PartitionSpec as P

F32 = jnp.float32
BF16 = jnp.bfloat16
MESH = pl.DeviceIdType.MESH


def largest_tile(size, limit):
    tile = limit
    while size % tile:
        tile //= 2
    return tile


def plan(n_gx, n_gy, nbf, rows, piece):
    s = type("Plan", (), {})()
    s.n_gx, s.n_gy, s.nbf, s.rows, s.piece = n_gx, n_gy, nbf, rows, piece
    s.bits = int(math.log2(n_gx)) - 1
    assert 2 << s.bits == n_gx and s.bits >= 1
    s.chips = n_gx // 2
    s.halves = 2 if piece % 256 == 0 else 1
    s.cw = piece // s.halves
    s.plane = nbf // n_gy
    s.strip = s.plane // n_gx
    s.mb = nbf // n_gx
    s.ch = 128 * s.bits
    s.chunks = nbf // s.ch
    s.per_plane = s.plane // s.ch
    s.units = sorted(
        ((r, h) for r in range(n_gx) for h in range(s.halves)),
        key=lambda u: (bin(u[0] >> 1).count("1"), u[1] if u[0] > 1 else 0, u[0] & 1, u[0], u[1]),
    )
    s.k_all = n_gx * piece
    s.k_half = s.k_all // 2
    s.t_rows = max(rows, nbf // 2 + 2 * s.ch)
    s.pt = largest_tile(rows, 1024)
    s.sorted_rows = s.mb % 128 == 0
    s.tt = largest_tile(nbf // 2, 768) if s.sorted_rows else s.mb
    s.near = [sorted((p for p in range(n_gy) if p != m), key=lambda p: (abs(p - m), p))
              for m in range(n_gy)]
    s.zr = largest_tile(rows, 128)
    return s


def last_bit(s, p, d):
    order = [(p + t) % s.bits for t in range(s.bits)]
    return [q for q in order if d >> q & 1][-1]


def kernel_body(s, coll, dens, zk, out, dfull, gath, upart, coll_v, dt, w, gbuf, r0, r1, rz, zin, zf,
                keep, ks, uf, sem_up, sem_z, sem_zs, sem_d, sem_ds, sem_g, sem_gs, sem_l, sem_gu, sem_zin,
                sem_rd, sem_rds, sem_rs, sem_rss, sem_rz, sem_rzs, sem_lc, sem_ld, ready):
    i, j = lax.axis_index("gx"), lax.axis_index("gy")
    bits, nbf, halves, cw, ch, mb = s.bits, s.nbf, s.halves, s.cw, s.ch, s.mb
    bit = [lax.rem(i // (1 << t), 2) for t in range(bits + 1)]

    def flip(mask):
        index = i
        for t in range(bits + 1):
            if mask >> t & 1:
                index = index + (1 - 2 * bit[t]) * (1 << t)
        return index

    def near_plane(t):
        plane = 0
        for m in range(s.n_gy):
            plane = plane + jnp.where(j == m, s.near[m][t - 1], 0)
        return plane

    def rows_at(start, size, unit=8):
        return pl.ds(pl.multiple_of(start, unit), size)

    def remote(src, dst, send, recv, gx, gy):
        return pltpu.make_async_remote_copy(
            src_ref=src, dst_ref=dst, send_sem=send, recv_sem=recv,
            device_id=(gx, gy), device_id_type=MESH)

    def hop(p, r):
        if r & 1:
            return r - 1, 1
        q = last_bit(s, p, r >> 1)
        return r - (2 << q), 2 << q

    own_cols = j * s.piece

    def own_piece(h, rws):
        return coll.at[rws, rows_at(own_cols + h * cw, cw, 128)]

    part_rows = nbf // bits

    def g_copy(h, p, r):
        src_r, mask = hop(p, r)
        rws = pl.ds(p * part_rows, part_rows)
        src = own_piece(h, rws) if src_r == 0 else gath.at[src_r * halves + h, rws]
        return remote(src, gath.at[r * halves + h, rws],
                      sem_gs.at[h, p, r], sem_g.at[h, p, r], flip(mask), j)

    def d_copy(t, p, r):
        src_r, mask = hop(p, r)
        start = near_plane(t) * s.plane + flip(src_r) * s.strip
        ref = dfull.at[rows_at(start, s.strip), pl.ds(p * part_rows, part_rows)]
        return remote(ref, ref, sem_ds.at[t, p, r], sem_d.at[t, p, r], flip(mask), j)

    inner = jnp.logical_and(j > 0, j < s.n_gy - 1)

    def part_cols(p):
        return pl.ds(p * part_rows, part_rows)

    def strip_rows(plane, p):
        return dfull.at[rows_at(plane * s.plane + i * s.strip, s.strip), part_cols(p)]

    def z_copy(t, step, p):
        plane = near_plane(t) if t else j
        src = strip_rows(plane, p) if t else dens.at[rows_at(i * s.strip, s.strip), part_cols(p)]
        return remote(src, strip_rows(plane, p), sem_zs.at[2 * t + (step > 0), p],
                      sem_z.at[plane, p], i, j + step)

    def z_sends(act):
        for step in (1, -1):
            @pl.when(j + step < s.n_gy if step > 0 else j > 0)
            def _():
                for p in range(bits):
                    act(z_copy(0, step, p))

    def z_relays(t, p, act):
        for step in (1, -1):
            plane = near_plane(t)

            @pl.when(jnp.logical_and(inner, plane < j if step > 0 else plane > j))
            def _():
                act(z_copy(t, step, p))

    def z_arrived(t, p):
        plane = near_plane(t)
        ref = strip_rows(plane, p)
        remote(ref, ref, sem_zs.at[0, p], sem_z.at[plane, p], i, plane).wait_recv()

    def onward(make, d, p):
        for r in range(2, s.n_gx, 2):
            if hop(p, r)[0] == 2 * d:
                make(p, r).start()
        make(p, 2 * d + 1).start()

    z_sends(lambda copy: copy.start())
    core = bit[0]

    def sorted_blocks():
        if not s.sorted_rows:
            return [(0, 0, nbf)]
        places = []
        for side in range(2):
            for q in range(s.chips):
                places.append((side * (nbf // 2) + q * mb, (2 * q + (1 - core if side == 0 else core)) * mb, mb))
        return places

    places = sorted_blocks()
    load_coll = [pltpu.make_async_copy(coll.at[rows_at(src, size, 128)], coll_v.at[pl.ds(at, size)],
                                       sem_lc.at[e]) for e, (at, src, size) in enumerate(places)]

    def load_density(ref, row):
        return [pltpu.make_async_copy(ref.at[rows_at(row, s.plane, 128), rows_at(src, size, 128)],
                                      r0.at[pl.ds(0, s.plane), pl.ds(at, size)], sem_ld.at[e])
                for e, (at, src, size) in enumerate(places)]

    for copy in load_coll + load_density(dens, 0):
        copy.start()
    for p in range(bits):
        g_copy(0, p, 2 << p).start()
    for h in range(halves):
        for p in range(bits):
            g_copy(h, p, 1).start()

    rt = largest_tile(s.plane, 256) if s.plane % 384 else 384

    def dense(mu0):
        def step(n, carry):
            a, t = lax.rem(n, s.plane // rt), n // (s.plane // rt)
            block = jnp.dot(r0[rows_at(a * rt, rt, 128), :], coll_v[:, rows_at(t * s.pt, s.pt, 128)],
                            preferred_element_type=F32)
            dt[rows_at(t * s.pt, s.pt, 128), rows_at(mu0 + a * rt, rt, 128)] = block.T.astype(BF16)
            return carry
        lax.fori_loop(0, (s.plane // rt) * (s.rows // s.pt), step, 0)

    def z_load(n):
        return pltpu.make_async_copy(zk.at[rows_at(n * s.zr, s.zr)], zin.at[lax.rem(n, 2)],
                                     sem_zin.at[lax.rem(n, 2)])

    steps = s.rows // s.zr

    def spread_kernel(first, last):
        lanes = s.piece // 128

        def step(n, carry):
            @pl.when(n + 1 < steps)
            def _():
                z_load(n + 1).start()
            z_load(n).wait()
            block = zin[lax.rem(n, 2)].astype(F32).reshape(s.zr * s.n_gx, s.piece)
            for c in range(lanes):
                zf[c] = block[:, c * 128:(c + 1) * 128]
            for u, (r, h) in enumerate(s.units):
                k = flip(r)
                for c in range(cw // 128):
                    lane = zf[h * (cw // 128) + c, pl.ds(k, s.zr, stride=s.n_gx), :]
                    w[rows_at(n * s.zr, s.zr, 16), pl.ds(u * cw + c * 128, 128)] = lane.astype(BF16)
            return carry
        lax.fori_loop(first, last, step, 0)

    z_load(0).start()
    for copy in load_coll + load_density(dens, 0):
        copy.wait()
    dense(j * s.plane)

    chip_order = sorted(range(1, s.chips), key=lambda d: (bin(d).count("1"), d))

    def strip_on(t):
        for p in range(bits):
            z_arrived(t, p)
            z_relays(t, p, lambda copy: copy.start())
            onward(functools.partial(d_copy, t), 0, p)

    def strips_on(t):
        for d in chip_order:
            for p in sorted(range(bits), key=lambda p: hop(p, 2 * d)[0]):
                d_copy(t, p, 2 * d).wait_recv()
                onward(functools.partial(d_copy, t), d, p)

    def dense_of(t):
        for d in range(s.chips):
            for p in range(bits):
                d_copy(t, p, 2 * d + 1).wait_recv()
        mu0 = near_plane(t) * s.plane
        for copy in load_density(dfull, mu0):
            copy.start()
        for copy in load_density(dfull, mu0):
            copy.wait()
        dense(mu0)

    for t in range(1, s.n_gy):
        if t in (2, 3):
            pl.when(inner)(lambda: strip_on(t))
            spread_kernel((t - 2) * steps // 2, (t - 1) * steps // 2)
            pl.when(jnp.logical_not(inner))(lambda: strip_on(t))
        else:
            strip_on(t)
        if t >= 2:
            strips_on(t - 1)
        if t >= 3:
            dense_of(t - 2)
    if s.n_gy < 4:
        spread_kernel(max(s.n_gy - 2, 0) * steps // 2, steps)
    strips_on(s.n_gy - 1)
    for h in range(halves):
        for p in range(bits):
            if h > 0:
                g_copy(h, p, 2 << p).start()
        for p in range(bits):
            for q in range(bits):
                if q != p:
                    g_copy(h, p, 2 << q).start()
    for t in range(max(1, s.n_gy - 2), s.n_gy):
        dense_of(t)

    def fetch(u):
        r, h = s.units[u]
        slot = gbuf.at[u % 2, pl.ds(0, nbf), pl.ds(0, cw)]
        if r == 0:
            src = own_piece(h, pl.ds(0, nbf))
        else:
            src = gath.at[r * halves + h]
        return pltpu.make_async_copy(src, slot, sem_l.at[2 + u % 2])

    n_units, tiles, half = len(s.units), s.rows // s.pt, len(s.units) // 2
    ahead = 4

    def by_link(u):
        return 0 < u < n_units and s.units[u][0] > 1 and not s.units[u][0] & 1

    def pass_on(u):
        r, h = s.units[u]
        for p in range(bits):
            g_copy(h, p, r).wait_recv()
            onward(functools.partial(g_copy, h), r >> 1, p)

    def arrive(u):
        r, h = s.units[u]
        if r & 1:
            for p in range(bits):
                g_copy(h, p, r).wait_recv()
        fetch(u).start()

    def m_loop(first, last):
        def m_step(n, carry):
            u, t = n // tiles, lax.rem(n, tiles)
            slot = lax.rem(u, 2)

            @pl.when(t == 0)
            def _():
                pltpu.make_async_copy(gath.at[0], gbuf.at[slot, pl.ds(0, nbf), pl.ds(0, cw)],
                                      sem_l.at[2 + slot]).wait()

            for uu in range(first, last):
                onto = uu + ahead if by_link(uu + ahead) and (uu + ahead < last or last == n_units) else 0
                if onto or uu + 1 < last:
                    @pl.when(jnp.logical_and(t == tiles // 2, u == uu))
                    def _():
                        if onto:
                            pass_on(onto)
                        if uu + 1 < last:
                            arrive(uu + 1)

            products = jnp.dot(dt[rows_at(t * s.pt, s.pt, 128), :], gbuf[slot, :nbf, :cw],
                               preferred_element_type=F32)
            place = (rows_at(t * s.pt, s.pt, 128), rows_at(u * cw, cw, 128))
            w[place] = (w[place].astype(F32) * products).astype(BF16)
            return carry
        lax.fori_loop(first * tiles, last * tiles, m_step, 0)

    def chunk_plane(n):
        shift = n // s.per_plane + 1
        return lax.rem(j + shift, s.n_gy)

    def gu_copies(n, part, slot, buffer, row):
        nu0 = chunk_plane(n) * s.plane + lax.rem(n, s.per_plane) * ch
        rws = rows_at(nu0, ch, 128)
        for e in range(half):
            r, h = s.units[part * half + e]
            src = own_piece(h, rws) if r == 0 else gath.at[r * halves + h, rws]
            dst = buffer.at[rows_at(row + slot * ch, ch, 128), pl.ds(e * cw, cw)]
            yield pltpu.make_async_copy(src, dst, sem_gu.at[slot, e])

    def u_product(n, t, part, buffer, row):
        return lax.dot_general(
            w[rows_at(t * s.pt, s.pt, 128), pl.ds(part * s.k_half, s.k_half)],
            buffer[rows_at(row + lax.rem(n, 2) * ch, ch, 128), pl.ds(0, s.k_half)],
            (((1,), (1,)), ((), ())), preferred_element_type=F32)

    def half_u():
        def store(n, t):
            rws = rows_at(t * s.pt, s.pt, 128)
            return pltpu.make_async_copy(uf.at[rws], upart.at[n, rws], sem_up.at[t])

        for copy in gu_copies(0, 0, 0, r0, 0):
            copy.start()

        def step(n, carry):
            slot = lax.rem(n, 2)
            for copy in gu_copies(n, 0, slot, r0, 0):
                copy.wait()

            @pl.when(n + 1 < s.chunks)
            def _():
                for copy in gu_copies(n + 1, 0, 1 - slot, r0, 0):
                    copy.start()

            @pl.when(n == s.chunks // 2 - 1)
            def _():
                for u in range(half, half + ahead):
                    if by_link(u):
                        pass_on(u)

            def u_step(t, carry):
                @pl.when(n >= 1)
                def _():
                    store(n - 1, t).wait()
                uf[rows_at(t * s.pt, s.pt, 128), :] = u_product(n, t, 0, r0, 0)
                store(n, t).start()
                return carry
            lax.fori_loop(0, tiles, u_step, 0)
            return carry
        lax.fori_loop(0, s.chunks, step, 0)
        for t in range(tiles):
            store(s.chunks - 1, t).wait()

    for u in range(min(ahead, half)):
        if by_link(u):
            pass_on(u)
    arrive(0)
    m_loop(0, half)
    half_u()
    arrive(half)
    m_loop(half, n_units)

    masks = [1] + [2 << q for q in range(bits)]
    for t, mask in enumerate(masks):
        pl.semaphore_signal(ready.at[t], inc=1, device_id=(flip(mask), j), device_id_type=MESH)

    def load_u(n):
        return pltpu.make_async_copy(upart.at[n], uf, sem_up.at[0])

    for copy in gu_copies(0, 1, 0, dt, nbf // 2):
        copy.start()
    load_u(0).start()
    for t in range(bits + 1):
        pl.semaphore_wait(ready.at[t], 1)

    half_rows = nbf // 2
    send_d = gbuf.at[0, pl.ds(0, half_rows), pl.ds(0, ch)]
    u_v = gbuf.at[1, pl.ds(0, s.rows), pl.ds(0, ch)]
    send_at, at = [], half_rows
    for t in range(bits):
        size = (s.chips >> (t + 1)) * mb
        send_at.append((at, size))
        at += size
    sz_at = at
    sz = gbuf.at[0, pl.ds(sz_at, mb), pl.ds(0, ch)]
    assert sz_at + mb <= nbf
    recvs = [r0] + [r1[t] for t in range(bits - 1)]

    def cols(n):
        return rows_at(n * ch, ch, 128)

    def swap_copy(n):
        return remote(send_d, dt.at[pl.ds(0, half_rows), cols(n)], sem_rds.at[0], sem_rd.at[n],
                      flip(1), j)

    def halve_copy(n, t, p):
        q = (p + t) % bits
        at, size = send_at[t]
        return remote(gbuf.at[0, pl.ds(at, size), pl.ds(p * 128, 128)],
                      recvs[t].at[pl.ds(0, size), rows_at(n * ch + p * 128, 128, 128)],
                      sem_rss.at[t, p], sem_rs.at[n, t, p], flip(2 << q), j)

    def blocks(t, p):
        q = (p + t) % bits
        free = [f for f in range(bits) if f not in [(p + e) % bits for e in range(t)]]
        rest = [f for f in free if f != q]
        pairs = []
        for combo in range(1 << len(rest)):
            base = 0
            for e, f in enumerate(rest):
                base = base + (combo >> e & 1) * (1 << free.index(f))
            weight = 1 << free.index(q)
            mine = bit[q + 1]
            pairs.append((base + mine * weight, base + (1 - mine) * weight))
        return pairs

    def held(n, t, p, block):
        rws, lane = rows_at(block * mb, mb, 128), pl.ds(p * 128, 128)
        arrived = dt if t == 0 else recvs[t - 1]
        mine = keep if t == 0 else ks[t - 1]
        return mine[rws, lane] + arrived[rws, rows_at(n * ch + p * 128, 128, 128)].astype(F32)

    def halve(n, t):
        at, _ = send_at[t]
        for p in range(bits):
            lane = pl.ds(p * 128, 128)

            @pl.when(n >= 1)
            def _():
                halve_copy(n - 1, t, p).wait_send()
            for e, (_, sent) in enumerate(blocks(t, p)):
                gbuf[0, pl.ds(at + e * mb, mb), lane] = held(n, t, p, sent).astype(BF16)
            halve_copy(n, t, p).start()
        for p in range(bits):
            for e, (kept, _) in enumerate(blocks(t, p)):
                ks[t][pl.ds(e * mb, mb), pl.ds(p * 128, 128)] = held(n, t, p, kept)

    def take(n, t):
        for p in range(bits):
            halve_copy(n, t, p).wait_recv()

    def plane_copy(n):
        shift = n // s.per_plane + 1
        c = lax.rem(n, s.per_plane)
        dst = rz.at[rows_at((shift - 1) * mb, mb, 8), rows_at(c * ch, ch, 128)]
        return remote(sz, dst, sem_rzs.at[0], sem_rz.at[n], i, chunk_plane(n))

    away = (s.n_gy - 1) * s.per_plane

    def finish(n):
        total = ks[bits - 1]

        @pl.when(n < away)
        def _():
            @pl.when(n >= 1)
            def _():
                plane_copy(n - 1).wait_send()
            for p in range(bits):
                gbuf[0, pl.ds(sz_at, mb), pl.ds(p * 128, 128)] = held(n, bits, p, 0).astype(BF16)
            plane_copy(n).start()

        @pl.when(n >= away)
        def _():
            c = n - away
            for t in range(s.n_gy - 1):
                plane_copy(t * s.per_plane + c).wait_recv()
            for p in range(bits):
                block = held(n, bits, p, 0)
                for t in range(s.n_gy - 1):
                    block += rz[pl.ds(t * mb, mb), rows_at(c * ch + p * 128, 128, 128)].astype(F32)
                total[pl.ds(0, mb), pl.ds(p * 128, 128)] = block
            copy = pltpu.make_async_copy(total.at[pl.ds(0, mb)], out.at[:, cols(c)], sem_l.at[0])
            copy.start()
            copy.wait()

    def b_step(n, carry):
        @pl.when(n < s.chunks)
        def _():
            slot = lax.rem(n, 2)
            for copy in gu_copies(n, 1, slot, dt, nbf // 2):
                copy.wait()

            @pl.when(n + 1 < s.chunks)
            def _():
                for copy in gu_copies(n + 1, 1, 1 - slot, dt, nbf // 2):
                    copy.start()
            load_u(n).wait()

            def u_step(t, carry):
                rws = rows_at(t * s.pt, s.pt, 128)
                gbuf[1, rws, pl.ds(0, ch)] = (
                    uf[rws, :] + u_product(n, t, 1, dt, nbf // 2)).astype(BF16)
                return carry
            lax.fori_loop(0, tiles, u_step, 0)

            @pl.when(n + 1 < s.chunks)
            def _():
                load_u(n + 1).start()

        for t in reversed(range(bits)):
            m = n - 2 - t

            @pl.when(jnp.logical_and(m >= 0, m < s.chunks))
            def _():
                take(m, t)
                if t == bits - 1:
                    finish(m)
                else:
                    halve(m, t + 1)

        @pl.when(jnp.logical_and(n >= 1, n <= s.chunks))
        def _():
            swap_copy(n - 1).wait()
            halve(n - 1, 0)

        @pl.when(n < s.chunks)
        def _():
            def t_block(q, side):
                if s.sorted_rows:
                    at = side * half_rows + q * s.tt
                else:
                    at = (2 * q + (1 - core if side == 0 else core)) * mb
                return jnp.dot(coll_v[rows_at(at, s.tt, 64), :],
                               gbuf[1, pl.ds(0, s.rows), pl.ds(0, ch)], preferred_element_type=F32)

            def sent(q, carry):
                gbuf[0, rows_at(q * s.tt, s.tt, 64), pl.ds(0, ch)] = t_block(q, 0).astype(BF16)
                return carry
            lax.fori_loop(0, half_rows // s.tt, sent, 0)
            swap_copy(n).start()

            def kept(q, carry):
                keep[rows_at(q * s.tt, s.tt, 64), :] = t_block(q, 1)
                return carry
            lax.fori_loop(0, half_rows // s.tt, kept, 0)
        return carry
    lax.fori_loop(0, s.chunks + bits + 1, b_step, 0)

    plane_copy(away - 1).wait_send()
    for t in range(bits):
        for p in range(bits):
            halve_copy(s.chunks - 1, t, p).wait_send()
    z_sends(lambda copy: copy.wait_send())
    for t in range(1, s.n_gy):
        for p in range(bits):
            z_relays(t, p, lambda copy: copy.wait_send())
    for r in range(1, s.n_gx):
        for p in range(bits):
            for t in range(1, s.n_gy):
                d_copy(t, p, r).wait_send()
            for h in range(halves):
                g_copy(h, p, r).wait_send()


def build(n_gx, n_gy):
    def local(collocation, density, kernel):
        nbf, rows = collocation.shape
        s = plan(n_gx, n_gy, nbf, rows, kernel.shape[3])
        zk = kernel.reshape(rows, n_gx, kernel.shape[3])
        any_spec = pl.BlockSpec(memory_space=pl.ANY)
        dma = pltpu.SemaphoreType.DMA
        wide = max(s.cw, s.ch)
        r1 = [pltpu.VMEM(((s.chips >> (t + 1)) * s.mb, nbf), BF16) for t in range(1, s.bits)]
        ks = [pltpu.VMEM(((s.chips >> (t + 1)) * s.mb, s.ch), F32) for t in range(s.bits)]
        out = pl.pallas_call(
            functools.partial(kernel_body, s),
            out_shape=(
                jax.ShapeDtypeStruct((s.mb, s.plane), F32),
                jax.ShapeDtypeStruct((nbf, nbf), BF16),
                jax.ShapeDtypeStruct((n_gx * s.halves, nbf, s.cw), BF16),
                jax.ShapeDtypeStruct((s.chunks, rows, s.ch), F32),
            ),
            in_specs=[any_spec] * 3,
            out_specs=(any_spec,) * 4,
            scratch_shapes=[
                pltpu.VMEM((nbf, rows), BF16),
                pltpu.VMEM((s.t_rows, nbf), BF16),
                pltpu.VMEM((rows, s.k_all), BF16),
                pltpu.VMEM((2, nbf, wide), BF16),
                pltpu.VMEM((max(s.plane, (s.chips // 2) * s.mb), nbf), BF16),
                r1,
                pltpu.VMEM(((n_gy - 1) * s.mb, s.plane), BF16),
                pltpu.VMEM((2, s.zr, n_gx, s.piece), BF16),
                pltpu.VMEM((s.piece // 128, s.zr * n_gx, 128), F32),
                pltpu.VMEM((nbf // 2, s.ch), F32),
                ks,
                pltpu.VMEM((rows, s.ch), F32),
                dma((rows // s.pt,)),
                dma((n_gy, s.bits)),
                dma((2 * n_gy, s.bits)),
                dma((n_gy, s.bits, n_gx)),
                dma((n_gy, s.bits, n_gx)),
                dma((s.halves, s.bits, n_gx)),
                dma((s.halves, s.bits, n_gx)),
                dma((4,)),
                dma((2, len(s.units) // 2)),
                dma((2,)),
                dma((s.chunks,)),
                dma((1,)),
                dma((s.chunks, s.bits, s.bits)),
                dma((s.bits, s.bits)),
                dma((s.chunks,)),
                dma((1,)),
                dma((n_gx,)),
                dma((n_gx,)),
                pltpu.SemaphoreType.REGULAR((s.bits + 1,)),
            ],
            compiler_params=pltpu.CompilerParams(
                has_side_effects=True, vmem_limit_bytes=67043328),
            name="exchange",
        )(collocation, density, zk)
        return out[0]

    return local


def solution(mesh):
    return jax.shard_map(
        build(mesh.shape["gx"], mesh.shape["gy"]),
        mesh=mesh,
        in_specs=(P(None, "gx"), P("gy", None), P("gx", None, "gy", None)),
        out_specs=P("gx", "gy"),
        check_vma=False,
    )
```
